32 devices in a mesh: groups: 2 (over x), blk: 8 (over z, y), sub: 2 (over core).
Axes of the slice: x: 2, y: 2, z: 4, core: 2. Of those that a mesh axis runs over, the one named last changes fastest.
Arguments:
- embeddings: bfloat16 [6144, 1024], P(('groups', 'blk', 'sub')), parts along dimension 0, may hold values from -6 to 6
- member_key: int32 [6144], P(('groups', 'blk', 'sub')), parts along dimension 0, may hold values from 0 to 1073741823, as said below
- limit_index: int32 [2], P('groups'), parts along dimension 0, may hold values from 0 to 7
Outputs:
- max_cosine: float32 [6144], P(('groups', 'blk', 'sub')), parts along dimension 0
- kept_share: float32 [2], P('groups'), parts along dimension 0
The draws below stay inside these ranges and needn't reach their ends.
There are 2 independent parts, one for each index of `groups`. The reference program is written for one: setup_inputs(seed, part) draws one part's arguments, and reference() takes and returns one part's arrays. A program takes and returns all parts, laid end to end along the dimension named above; each array names one. Nothing has to cross between parts.
Inputs may be any that keep to these rules, and one draw needn't show every extreme that they name: `member_key`: all keys of a cluster are distinct. A key's quotient by 268435456 is the member's sub-cluster, 0 to 3; its remainder orders the members.
All inputs are finite; a program needn't handle non-finite values.
Results may differ from the reference program's by a relative error of at most 0.0013.
Values may be sent and summed in bfloat16 or wider, within the bound.
A program may use at most 64 MiB of HBM per device.

```python
import math
import jax
import jax.numpy as jnp
from jax import lax

D = 1024
LABELS = 4
LIMITS = 8
MEMBERS = 3072


label_stride = 268435456


def draw_member_key(key, part):
    spacing = label_stride // MEMBERS
    places = jax.random.permutation(jax.random.fold_in(key, 11), MEMBERS).astype(jnp.int32)
    jitter = jax.random.randint(jax.random.fold_in(key, 12), (MEMBERS,), 0, spacing, dtype=jnp.int32)
    labels = jax.random.randint(jax.random.fold_in(key, 13), (MEMBERS,), 0, LABELS, dtype=jnp.int32)
    return labels * label_stride + places * spacing + jitter


def levels(rng, shape, pieces, low, top_value):
    gain, own = 1.0, jax.random.fold_in(rng, 6)
    for position, parts in pieces:
        heights = jnp.exp(jax.random.uniform(jax.random.fold_in(own, position), (parts,), jnp.float32, low / len(pieces), top_value / len(pieces)))
        gain = gain * jnp.repeat(heights, shape[position] // parts).reshape([-1 if axis == position else 1 for axis in range(len(shape))])
    return gain


def noise(rng, extent, spread, bound, split=(), kind=jnp.bfloat16):
    factor_of = levels(rng, extent, split, -0.22, 0.18) if split else 1.0
    entries = jax.random.normal(rng, extent, jnp.float32) * spread * factor_of
    return jnp.minimum(jnp.maximum(entries, -bound), bound).astype(kind)


def setup_inputs(seed: int = 0, part: int = 0) -> dict:
    key_of = jax.random.split(jax.random.key(seed), 4)
    own_keys = jax.random.split(jax.random.fold_in(key_of[3], part), 4)
    embeddings = noise(own_keys[0], (MEMBERS, D), 1.0, 6.0, ((0, 16),))
    member_key = draw_member_key(jax.random.fold_in(jax.random.fold_in(key_of[3], part), 71), part)
    limit_index = jax.random.randint(own_keys[2], (1,), 0, LIMITS).astype(jnp.int32)
    return {"embeddings": embeddings, "member_key": member_key, "limit_index": limit_index}


label_stride = 268435456

def normalize(embeddings):
    values = embeddings.astype(jnp.float32)
    mean_square = lax.optimization_barrier(jnp.mean(values * values, axis=1, keepdims=True))
    scaled = values * lax.rsqrt(mean_square + 1e-06) * (1.0 / math.sqrt(values.shape[1]))
    return scaled.astype(jnp.bfloat16)

def reference(embeddings, member_key, limit_index):
    unit = normalize(embeddings)
    total = unit.shape[0]
    block_rows = math.gcd(total, 512)
    label_all = member_key // label_stride

    def one_block(index):
        begin = (index * block_rows).astype(jnp.int32)
        rows = lax.dynamic_slice_in_dim(unit, begin, block_rows, 0)
        keys = lax.dynamic_slice_in_dim(member_key, begin, block_rows, 0)
        labels = lax.dynamic_slice_in_dim(label_all, begin, block_rows, 0)
        scores = lax.dot_general(rows, unit, (((1,), (1,)), ((), ())), preferred_element_type=jnp.float32)
        allowed = (member_key[None, :] < keys[:, None]) & (label_all[None, :] == labels[:, None])
        return lax.optimization_barrier(jnp.max(jnp.where(allowed, scores, jnp.float32(-1.0)), axis=1))
    max_cosine = lax.map(one_block, jnp.arange(total // block_rows, dtype=jnp.int32)).reshape(total)
    width = math.sqrt(unit.shape[1])
    table = (2.0 + 0.5 * jnp.arange(LIMITS, dtype=jnp.float32)) / width
    limit = jnp.sum(jnp.where(jnp.arange(LIMITS, dtype=jnp.int32) == limit_index[0], table, jnp.float32(0.0)))
    kept = jax.nn.sigmoid(2.0 * width * (limit - max_cosine))
    kept_share = (jnp.sum(kept) / total).reshape(1)
    return (max_cosine, kept_share)
```

```python
import functools
import math

import jax
import jax.numpy as jnp
from jax import lax
from jax.experimental import pallas as pl
from jax.experimental.pallas import tpu as pltpu
from jax.sharding import PartitionSpec as P

MESH = pl.DeviceIdType.MESH
LANES = 128
label_stride = 268435456


def normalize(block):
    values = block.astype(jnp.float32)
    mean_square = jnp.mean(values * values, axis=1, keepdims=True)
    scaled = values * lax.rsqrt(mean_square + 1e-06) * (1.0 / math.sqrt(values.shape[1]))
    return scaled.astype(jnp.bfloat16)


def ring_place(index, n):
    odd = lax.rem(index, 2)
    return (1 - odd) * lax.div(index, 2) + odd * (n - 1 - lax.div(index, 2))


def ring_index(place, n):
    late = lax.div(place, n // 2)
    return (1 - late) * (2 * place) + late * (2 * (n - 1 - place) + 1)


def kernel(
    n, subs, reach, chunks,
    x_hbm, key_ref, limit_ref, best_ref, share_ref,
    left, right, unit_left, unit_right, keys,
    row_out, row_in, col_out, col_in, sums,
    load_sem, key_send, key_recv,
    up_send, up_recv, down_send, down_recv, side_send, side_recv,
    row_send, row_recv, col_send, col_recv, sum_send, sum_recv,
):
    rows, width = x_hbm.shape
    piece = rows // chunks
    blk = lax.axis_index("blk")
    sub = lax.axis_index("sub")
    place = ring_place(blk, n)

    def device(offset, sub_step):
        there = ring_index(lax.rem(place + offset + n, n), n)
        return {"blk": there, "sub": lax.rem(sub + sub_step, subs)}

    def remote(src, dst, send, recv, offset, sub_step):
        return pltpu.make_async_remote_copy(
            src_ref=src, dst_ref=dst, send_sem=send, recv_sem=recv,
            device_id=device(offset, sub_step), device_id_type=MESH,
        )

    load = pltpu.make_async_copy(x_hbm, right.at[0, sub], load_sem)
    load.start()

    others = [(o, s) for o in range(n) for s in range(subs) if (o, s) != (0, 0)]
    barrier = pltpu.get_barrier_semaphore()
    for o, s in others:
        pl.semaphore_signal(barrier, inc=1, device_id=device(o, s), device_id_type=MESH)
    keys[reach, sub] = key_ref[...]
    pl.semaphore_wait(barrier, len(others))

    load.wait()
    span = lambda k: pl.ds(k * piece, piece)
    up, down, side = {}, {}, {}
    for hop in range(1, reach + 1):
        for k in range(chunks):
            src = right.at[0, sub, span(k)] if hop == 1 else left.at[hop - 2, span(k)]
            up[hop, k] = remote(
                src, left.at[hop - 1, span(k)], up_send.at[hop - 1, k], up_recv.at[hop - 1, k], 1, 0
            )
            down[hop, k] = remote(
                right.at[hop - 1, sub, span(k)], right.at[hop, sub, span(k)],
                down_send.at[hop - 1, k], down_recv.at[hop - 1, k], -1, 0,
            )
    for hop in range(reach + 1):
        for k in range(chunks):
            for s in range(1, subs):
                here = right.at[hop, sub, span(k)]
                side[hop, k, s] = remote(
                    here, here, side_send.at[hop, k, s - 1], side_recv.at[hop, k, s - 1], 0, s
                )
    key_copies = [
        remote(
            key_ref, keys.at[reach - o, sub],
            key_send.at[reach - o, s], key_recv.at[reach - o, s], o, s,
        )
        for o in range(-reach, reach + 1) for s in range(subs) if (o, s) != (0, 0)
    ]

    for k in range(chunks):
        up[1, k].start()
        down[1, k].start()
    for k in range(chunks):
        for s in range(1, subs):
            side[0, k, s].start()
    for copy in key_copies:
        copy.start()

    unit_right[0, sub] = normalize(right[0, sub])
    for k in range(chunks):
        for s in range(1, subs):
            side[0, k, s].wait_recv()
    for s in range(1, subs):
        unit_right[0, lax.rem(sub + s, subs)] = normalize(right[0, lax.rem(sub + s, subs)])
    for copy in key_copies:
        copy.wait_recv()

    floor = jnp.float32(-1.0)
    wide = subs * rows
    best_row, best_col = {}, {}

    def compare(back, ahead):
        lhs = unit_right[0, sub] if back == 0 else unit_left[back - 1]
        rhs = unit_right[ahead].reshape(wide, width)
        scores = lax.dot_general(
            lhs, rhs, (((1,), (1,)), ((), ())), preferred_element_type=jnp.float32
        )
        row_key = jnp.broadcast_to(keys[reach - back, sub], (LANES, rows)).T
        col_key = jnp.concatenate([keys[reach + ahead, s] for s in range(subs)], axis=1)
        columns = []
        for start in range(0, wide, LANES):
            tile = scores[:, start : start + LANES]
            other = jnp.broadcast_to(col_key[:, start : start + LANES], (rows, LANES))
            same = jnp.where((row_key ^ other) < label_stride, tile, floor)
            earlier = other < row_key
            to_row = jnp.where(earlier, same, floor)
            best_row[back] = jnp.maximum(best_row[back], to_row) if back in best_row else to_row
            if ahead or back:
                columns.append(jnp.max(jnp.where(earlier, floor, same), axis=0, keepdims=True))
        if columns:
            column = jnp.concatenate(columns, axis=1)
            best_col[ahead] = (
                jnp.maximum(best_col[ahead], column) if ahead in best_col else column
            )

    def row_of(back):
        return jnp.max(best_row[back].T, axis=0, keepdims=True)

    pairs = [(d // 2, d - d // 2) for d in range(min(2 * reach, n // 2) + 1)]
    last_row = {b: max(i for i, p in enumerate(pairs) if p[0] == b) for b in {p[0] for p in pairs}}
    last_col = {a: max(i for i, p in enumerate(pairs) if p[1] == a) for a in {p[1] for p in pairs}}
    row_copies, col_copies = [], []

    def run(i):
        back, ahead = pairs[i]
        compare(back, ahead)
        if back and last_row[back] == i:
            row_out[back - 1] = row_of(back)
            copy = remote(
                row_out.at[back - 1], row_in.at[back - 1],
                row_send.at[back - 1], row_recv.at[back - 1], -back, 0,
            )
            copy.start()
            row_copies.append(copy)
        if ahead and last_col[ahead] == i:
            for s in range(subs):
                col_out[ahead - 1, s] = best_col[ahead][:, s * rows : (s + 1) * rows]
            for s in range(subs):
                target = lax.rem(sub + s, subs)
                copy = remote(
                    col_out.at[ahead - 1, target], col_in.at[ahead - 1, sub],
                    col_send.at[ahead - 1, s], col_recv.at[ahead - 1, s], ahead, s,
                )
                copy.start()
                col_copies.append(copy)

    run(0)
    done = 1
    for hop in range(1, reach + 1):
        for k in range(chunks):
            up[hop, k].wait_recv()
            if hop < reach:
                up[hop + 1, k].start()
            down[hop, k].wait_recv()
            if hop < reach:
                down[hop + 1, k].start()
            for s in range(1, subs):
                side[hop, k, s].start()
            unit_left[hop - 1, span(k)] = normalize(left[hop - 1, span(k)])
            unit_right[hop, sub, span(k)] = normalize(right[hop, sub, span(k)])
            for s in range(1, subs):
                side[hop, k, s].wait_recv()
                there = lax.rem(sub + s, subs)
                unit_right[hop, there, span(k)] = normalize(right[hop, there, span(k)])
        while done < len(pairs) and max(pairs[done]) <= hop:
            run(done)
            done += 1

    for copy in row_copies + col_copies:
        copy.wait_recv()
    best = jnp.maximum(row_of(0), floor)
    for back in last_row:
        if back:
            best = jnp.maximum(best, row_in[back - 1])
    for ahead in last_col:
        if ahead:
            for s in range(subs):
                best = jnp.maximum(best, col_in[ahead - 1, s])
    best_ref[...] = best

    scale = math.sqrt(width)
    limit = (2.0 + 0.5 * jnp.full((1, rows), limit_ref[0], jnp.int32).astype(jnp.float32)) / scale
    kept = jax.nn.sigmoid(2.0 * scale * (limit - best))
    total = jnp.sum(kept, axis=1, keepdims=True)
    sums[blk, sub] = jnp.broadcast_to(total, (1, LANES))
    sum_copies = [
        remote(
            sums.at[blk, sub], sums.at[blk, sub],
            sum_send.at[o, s], sum_recv.at[o, s], o, s,
        )
        for o, s in others
    ]
    for copy in sum_copies:
        copy.start()
    for copies in (up, down, side):
        for copy in copies.values():
            copy.wait_send()
    for copy in key_copies + row_copies + col_copies:
        copy.wait_send()
    for copy in sum_copies:
        copy.wait_recv()
    everything = jnp.sum(sums[...].reshape(n * subs, LANES), axis=0, keepdims=True)
    share_ref[...] = (everything / (n * subs * rows))[:, :1]
    for copy in sum_copies:
        copy.wait_send()


def solution(mesh):
    n, subs = mesh.shape["blk"], mesh.shape["sub"]

    def on_device(embeddings, member_key, limit_index):
        rows, width = embeddings.shape
        reach = -(-(n // 2) // 2)
        chunks = 4 if rows % 64 == 0 else 1
        dma = pltpu.SemaphoreType.DMA
        raw, f32, i32 = embeddings.dtype, jnp.float32, jnp.int32
        held = (2 * reach + 1 + (2 * reach + 2) * (subs - 1)) * 2
        best, share = pl.pallas_call(
            functools.partial(kernel, n, subs, reach, chunks),
            out_shape=(
                jax.ShapeDtypeStruct((1, rows), f32),
                jax.ShapeDtypeStruct((1, 1), f32),
            ),
            in_specs=[
                pl.BlockSpec(memory_space=pl.ANY),
                pl.BlockSpec(memory_space=pltpu.VMEM),
                pl.BlockSpec(memory_space=pltpu.SMEM),
            ],
            out_specs=(
                pl.BlockSpec(memory_space=pltpu.VMEM),
                pl.BlockSpec(memory_space=pltpu.VMEM),
            ),
            scratch_shapes=[
                pltpu.VMEM((reach, rows, width), raw),
                pltpu.VMEM((reach + 1, subs, rows, width), raw),
                pltpu.VMEM((reach, rows, width), jnp.bfloat16),
                pltpu.VMEM((reach + 1, subs, rows, width), jnp.bfloat16),
                pltpu.VMEM((2 * reach + 1, subs, 1, rows), i32),
                pltpu.VMEM((reach, 1, rows), f32),
                pltpu.VMEM((reach, 1, rows), f32),
                pltpu.VMEM((reach, subs, 1, rows), f32),
                pltpu.VMEM((reach, subs, 1, rows), f32),
                pltpu.VMEM((n, subs, 1, LANES), f32),
                dma,
                dma((2 * reach + 1, subs)),
                dma((2 * reach + 1, subs)),
                dma((reach, chunks)),
                dma((reach, chunks)),
                dma((reach, chunks)),
                dma((reach, chunks)),
                dma((reach + 1, chunks, max(subs - 1, 1))),
                dma((reach + 1, chunks, max(subs - 1, 1))),
                dma((reach,)),
                dma((reach,)),
                dma((reach, subs)),
                dma((reach, subs)),
                dma((n, subs)),
                dma((n, subs)),
            ],
            compiler_params=pltpu.CompilerParams(
                collective_id=0,
                has_side_effects=True,
                vmem_limit_bytes=held * rows * width * 2 + 16 * 2**20,
            ),
        )(embeddings, member_key.reshape(1, rows), limit_index)
        return best.reshape(rows), share.reshape(1)

    in_specs = (P(("groups", "blk", "sub"), None), P(("groups", "blk", "sub")), P("groups"))
    out_specs = (P(("groups", "blk", "sub")), P("groups"))
    return jax.shard_map(
        on_device, mesh=mesh, in_specs=in_specs, out_specs=out_specs, check_vma=False
    )
```

```python
import functools
import math

import jax
import jax.numpy as jnp
from jax import lax
from jax.experimental import pallas as pl
from jax.experimental.pallas import tpu as pltpu
from jax.sharding import PartitionSpec as P

MESH = pl.DeviceIdType.MESH
LANES = 128
label_stride = 268435456


def normalize(block):
    values = block.astype(jnp.float32)
    mean_square = jnp.mean(values * values, axis=1, keepdims=True)
    scaled = values * lax.rsqrt(mean_square + 1e-06) * (1.0 / math.sqrt(values.shape[1]))
    return scaled.astype(jnp.bfloat16)


def ring_place(index, n):
    odd = lax.rem(index, 2)
    return (1 - odd) * lax.div(index, 2) + odd * (n - 1 - lax.div(index, 2))


def ring_index(place, n):
    late = lax.div(place, n // 2)
    return (1 - late) * (2 * place) + late * (2 * (n - 1 - place) + 1)


def kernel(
    n, subs, reach, chunks,
    x_hbm, key_hbm, limit_ref, best_ref, share_ref,
    left, right, unit_left, unit_right, keys,
    row_out, row_in, col_out, col_in, sums,
    load_sem, key_send, key_recv,
    up_send, up_recv, down_send, down_recv, side_send, side_recv,
    row_send, row_recv, col_send, col_recv, sum_send, sum_recv,
):
    rows, width = x_hbm.shape
    piece = rows // chunks
    blk = lax.axis_index("blk")
    sub = lax.axis_index("sub")
    place = ring_place(blk, n)

    def device(offset, sub_step):
        there = ring_index(lax.rem(place + offset + n, n), n)
        return {"blk": there, "sub": lax.rem(sub + sub_step, subs)}

    def remote(src, dst, send, recv, offset, sub_step):
        return pltpu.make_async_remote_copy(
            src_ref=src, dst_ref=dst, send_sem=send, recv_sem=recv,
            device_id=device(offset, sub_step), device_id_type=MESH,
        )

    load = pltpu.make_async_copy(x_hbm, right.at[0, sub], load_sem.at[0])
    load.start()
    load_key = pltpu.make_async_copy(key_hbm, keys.at[reach, sub], load_sem.at[1])
    load_key.start()

    others = [(o, s) for o in range(n) for s in range(subs) if (o, s) != (0, 0)]
    near = [(1, 0), (-1, 0)] + [(0, s) for s in range(1, subs)]
    barrier = pltpu.get_barrier_semaphore()
    for o, s in near:
        pl.semaphore_signal(barrier, inc=1, device_id=device(o, s), device_id_type=MESH)
    pl.semaphore_wait(barrier, len(near))

    load.wait()
    load_key.wait()
    span = lambda k: pl.ds(k * piece, piece)
    up, down, side = {}, {}, {}
    for hop in range(1, reach + 1):
        for k in range(chunks):
            src = right.at[0, sub, span(k)] if hop == 1 else left.at[hop - 2, span(k)]
            up[hop, k] = remote(
                src, left.at[hop - 1, span(k)], up_send.at[hop - 1, k], up_recv.at[hop - 1, k], 1, 0
            )
            down[hop, k] = remote(
                right.at[hop - 1, sub, span(k)], right.at[hop, sub, span(k)],
                down_send.at[hop - 1, k], down_recv.at[hop - 1, k], -1, 0,
            )
    for hop in range(reach + 1):
        for k in range(chunks):
            for s in range(1, subs):
                here = right.at[hop, sub, span(k)]
                side[hop, k, s] = remote(
                    here, here, side_send.at[hop, k, s - 1], side_recv.at[hop, k, s - 1], 0, s
                )
    key_up, key_down, key_side = {}, {}, {}
    for hop in range(1, reach + 1):
        for table, way in ((key_up, -1), (key_down, 1)):
            table[hop] = remote(
                keys.at[reach + way * (hop - 1), sub], keys.at[reach + way * hop, sub],
                key_send.at[reach + way * hop, 0], key_recv.at[reach + way * hop, 0], -way, 0,
            )
    for hop in range(reach + 1):
        for s in range(1, subs):
            here = keys.at[reach + hop, sub]
            key_side[hop, s] = remote(
                here, here, key_send.at[reach + hop, s], key_recv.at[reach + hop, s], 0, s
            )

    key_up[1].start()
    key_down[1].start()
    for k in range(chunks):
        up[1, k].start()
        down[1, k].start()
    for k in range(chunks):
        for s in range(1, subs):
            side[0, k, s].start()
    for s in range(1, subs):
        key_side[0, s].start()

    unit_right[0, sub] = normalize(right[0, sub])
    for k in range(chunks):
        for s in range(1, subs):
            side[0, k, s].wait_recv()
    for s in range(1, subs):
        unit_right[0, lax.rem(sub + s, subs)] = normalize(right[0, lax.rem(sub + s, subs)])
        key_side[0, s].wait_recv()

    floor = jnp.float32(-1.0)
    wide = subs * rows
    best_row, best_col = {}, {}

    def compare(back, ahead):
        lhs = unit_right[0, sub] if back == 0 else unit_left[back - 1]
        rhs = unit_right[ahead].reshape(wide, width)
        scores = lax.dot_general(
            lhs, rhs, (((1,), (1,)), ((), ())), preferred_element_type=jnp.float32
        )
        row_key = jnp.broadcast_to(keys[reach - back, sub], (LANES, rows)).T
        col_key = jnp.concatenate([keys[reach + ahead, s] for s in range(subs)], axis=1)
        columns = []
        for start in range(0, wide, LANES):
            tile = scores[:, start : start + LANES]
            other = jnp.broadcast_to(col_key[:, start : start + LANES], (rows, LANES))
            same = jnp.where((row_key ^ other) < label_stride, tile, floor)
            earlier = other < row_key
            to_row = jnp.where(earlier, same, floor)
            best_row[back] = jnp.maximum(best_row[back], to_row) if back in best_row else to_row
            if ahead or back:
                columns.append(jnp.max(jnp.where(earlier, floor, same), axis=0, keepdims=True))
        if columns:
            column = jnp.concatenate(columns, axis=1)
            best_col[ahead] = (
                jnp.maximum(best_col[ahead], column) if ahead in best_col else column
            )

    def row_of(back):
        return jnp.max(best_row[back].T, axis=0, keepdims=True)

    pairs = [(d // 2, d - d // 2) for d in range(min(2 * reach, n // 2) + 1)]
    last_row = {b: max(i for i, p in enumerate(pairs) if p[0] == b) for b in {p[0] for p in pairs}}
    last_col = {a: max(i for i, p in enumerate(pairs) if p[1] == a) for a in {p[1] for p in pairs}}
    row_copies, col_copies = [], []

    def run(i):
        back, ahead = pairs[i]
        compare(back, ahead)
        if back and last_row[back] == i:
            row_out[back - 1] = row_of(back)
            copy = remote(
                row_out.at[back - 1], row_in.at[back - 1],
                row_send.at[back - 1], row_recv.at[back - 1], -back, 0,
            )
            copy.start()
            row_copies.append(copy)
        if ahead and last_col[ahead] == i:
            for s in range(subs):
                col_out[ahead - 1, s] = best_col[ahead][:, s * rows : (s + 1) * rows]
            for s in range(subs):
                target = lax.rem(sub + s, subs)
                copy = remote(
                    col_out.at[ahead - 1, target], col_in.at[ahead - 1, sub],
                    col_send.at[ahead - 1, s], col_recv.at[ahead - 1, s], ahead, s,
                )
                copy.start()
                col_copies.append(copy)

    run(0)
    done = 1
    for hop in range(1, reach + 1):
        key_up[hop].wait_recv()
        key_down[hop].wait_recv()
        if hop < reach:
            key_up[hop + 1].start()
            key_down[hop + 1].start()
        for s in range(1, subs):
            key_side[hop, s].start()
        for k in range(chunks):
            up[hop, k].wait_recv()
            if hop < reach:
                up[hop + 1, k].start()
            down[hop, k].wait_recv()
            if hop < reach:
                down[hop + 1, k].start()
            for s in range(1, subs):
                side[hop, k, s].start()
            unit_left[hop - 1, span(k)] = normalize(left[hop - 1, span(k)])
            unit_right[hop, sub, span(k)] = normalize(right[hop, sub, span(k)])
            for s in range(1, subs):
                side[hop, k, s].wait_recv()
                there = lax.rem(sub + s, subs)
                unit_right[hop, there, span(k)] = normalize(right[hop, there, span(k)])
        for s in range(1, subs):
            key_side[hop, s].wait_recv()
        while done < len(pairs) and max(pairs[done]) <= hop:
            run(done)
            done += 1

    for copy in row_copies + col_copies:
        copy.wait_recv()
    best = jnp.maximum(row_of(0), floor)
    for back in last_row:
        if back:
            best = jnp.maximum(best, row_in[back - 1])
    for ahead in last_col:
        if ahead:
            for s in range(subs):
                best = jnp.maximum(best, col_in[ahead - 1, s])
    best_ref[...] = best

    scale = math.sqrt(width)
    limit = (2.0 + 0.5 * jnp.full((1, rows), limit_ref[0], jnp.int32).astype(jnp.float32)) / scale
    kept = jax.nn.sigmoid(2.0 * scale * (limit - best))
    total = jnp.sum(kept, axis=1, keepdims=True)
    sums[blk, sub] = jnp.broadcast_to(total, (1, LANES))
    sum_copies = [
        remote(
            sums.at[blk, sub], sums.at[blk, sub],
            sum_send.at[o, s], sum_recv.at[o, s], o, s,
        )
        for o, s in others
    ]
    for copy in sum_copies:
        copy.start()
    for copies in (up, down, side, key_up, key_down, key_side):
        for copy in copies.values():
            copy.wait_send()
    for copy in row_copies + col_copies:
        copy.wait_send()
    for copy in sum_copies:
        copy.wait_recv()
    everything = jnp.sum(sums[...].reshape(n * subs, LANES), axis=0, keepdims=True)
    share_ref[...] = (everything / (n * subs * rows))[:, :1]
    for copy in sum_copies:
        copy.wait_send()


def solution(mesh):
    n, subs = mesh.shape["blk"], mesh.shape["sub"]

    def on_device(embeddings, member_key, limit_index):
        rows, width = embeddings.shape
        reach = -(-(n // 2) // 2)
        chunks = 4 if rows % 64 == 0 else 1
        dma = pltpu.SemaphoreType.DMA
        raw, f32, i32 = embeddings.dtype, jnp.float32, jnp.int32
        best, share = pl.pallas_call(
            functools.partial(kernel, n, subs, reach, chunks),
            out_shape=(
                jax.ShapeDtypeStruct((1, rows), f32),
                jax.ShapeDtypeStruct((1, 1), f32),
            ),
            in_specs=[
                pl.BlockSpec(memory_space=pltpu.HBM),
                pl.BlockSpec(memory_space=pltpu.HBM),
                pl.BlockSpec(memory_space=pltpu.SMEM),
            ],
            out_specs=(
                pl.BlockSpec(memory_space=pltpu.VMEM),
                pl.BlockSpec(memory_space=pltpu.VMEM),
            ),
            scratch_shapes=[
                pltpu.VMEM((reach, rows, width), raw),
                pltpu.VMEM((reach + 1, subs, rows, width), raw),
                pltpu.VMEM((reach, rows, width), jnp.bfloat16),
                pltpu.VMEM((reach + 1, subs, rows, width), jnp.bfloat16),
                pltpu.VMEM((2 * reach + 1, subs, 1, rows), i32),
                pltpu.VMEM((reach, 1, rows), f32),
                pltpu.VMEM((reach, 1, rows), f32),
                pltpu.VMEM((reach, subs, 1, rows), f32),
                pltpu.VMEM((reach, subs, 1, rows), f32),
                pltpu.VMEM((n, subs, 1, LANES), f32),
                dma((2,)),
                dma((2 * reach + 1, subs)),
                dma((2 * reach + 1, subs)),
                dma((reach, chunks)),
                dma((reach, chunks)),
                dma((reach, chunks)),
                dma((reach, chunks)),
                dma((reach + 1, chunks, max(subs - 1, 1))),
                dma((reach + 1, chunks, max(subs - 1, 1))),
                dma((reach,)),
                dma((reach,)),
                dma((reach, subs)),
                dma((reach, subs)),
                dma((n, subs)),
                dma((n, subs)),
            ],
            compiler_params=pltpu.CompilerParams(
                collective_id=0,
                has_side_effects=True,
            ),
        )(embeddings, member_key.reshape(1, rows), limit_index)
        return best.reshape(rows), share.reshape(1)

    in_specs = (P(("groups", "blk", "sub"), None), P(("groups", "blk", "sub")), P("groups"))
    out_specs = (P(("groups", "blk", "sub")), P("groups"))
    return jax.shard_map(
        on_device, mesh=mesh, in_specs=in_specs, out_specs=out_specs, check_vma=False
    )
```

```python
import functools
import math

import jax
import jax.numpy as jnp
from jax import lax
from jax.experimental import pallas as pl
from jax.experimental.pallas import tpu as pltpu
from jax.sharding import PartitionSpec as P

MESH = pl.DeviceIdType.MESH
LANES = 128
label_stride = 268435456


def normalize(block):
    values = block.astype(jnp.float32)
    mean_square = jnp.mean(values * values, axis=1, keepdims=True)
    scaled = values * lax.rsqrt(mean_square + 1e-06) * (1.0 / math.sqrt(values.shape[1]))
    return scaled.astype(jnp.bfloat16)


def ring_place(index, n):
    odd = lax.rem(index, 2)
    return (1 - odd) * lax.div(index, 2) + odd * (n - 1 - lax.div(index, 2))


def ring_index(place, n):
    late = lax.div(place, n // 2)
    return (1 - late) * (2 * place) + late * (2 * (n - 1 - place) + 1)


def plan(n, reach):
    pairs = [(d // 2, d - d // 2) for d in range(min(2 * reach, n // 2) + 1)]
    last = [{p[side]: i for i, p in enumerate(pairs)} for side in (0, 1)]
    late = [[v for v, i in table.items() if v and max(pairs[i]) == reach] for table in last]
    return pairs, last[0], last[1], late[0], late[1]


def kernel(
    n, subs, reach, chunks,
    x_hbm, key_hbm, limit_ref, best_ref, share_ref,
    left, right, unit_left, unit_right, keys,
    row_out, row_in, col_out, col_in, table, maxima, ready,
    load_sem, key_send, key_recv,
    up_send, up_recv, down_send, down_recv, side_send, side_recv,
    row_send, row_recv, col_send, col_recv, sum_send, sum_recv,
):
    rows, width = x_hbm.shape
    piece = rows // chunks
    blk = lax.axis_index("blk")
    sub = lax.axis_index("sub")
    place = ring_place(blk, n)

    def device(offset, sub_step):
        there = ring_index(lax.rem(place + offset + n, n), n)
        return {"blk": there, "sub": lax.rem(sub + sub_step, subs)}

    def remote(src, dst, send, recv, offset, sub_step):
        return pltpu.make_async_remote_copy(
            src_ref=src, dst_ref=dst, send_sem=send, recv_sem=recv,
            device_id=device(offset, sub_step), device_id_type=MESH,
        )

    load = pltpu.make_async_copy(x_hbm, right.at[0, sub], load_sem.at[0])
    load.start()
    load_key = pltpu.make_async_copy(key_hbm, keys.at[reach, sub], load_sem.at[1])
    load_key.start()

    others = [(o, s) for o in range(n) for s in range(subs) if (o, s) != (0, 0)]
    near = [(1, 0), (-1, 0)] + [(0, s) for s in range(1, subs)]
    barrier = pltpu.get_barrier_semaphore()
    for o, s in near:
        pl.semaphore_signal(barrier, inc=1, device_id=device(o, s), device_id_type=MESH)
    pl.semaphore_wait(barrier, len(near))

    load.wait()
    load_key.wait()
    span = lambda k: pl.ds(k * piece, piece)
    up, down, side = {}, {}, {}
    for hop in range(1, reach + 1):
        for k in range(chunks):
            src = right.at[0, sub, span(k)] if hop == 1 else left.at[hop - 2, span(k)]
            up[hop, k] = remote(
                src, left.at[hop - 1, span(k)], up_send.at[hop - 1, k], up_recv.at[hop - 1, k], 1, 0
            )
            down[hop, k] = remote(
                right.at[hop - 1, sub, span(k)], right.at[hop, sub, span(k)],
                down_send.at[hop - 1, k], down_recv.at[hop - 1, k], -1, 0,
            )
    for hop in range(reach + 1):
        for k in range(chunks):
            for s in range(1, subs):
                here = right.at[hop, sub, span(k)]
                side[hop, k, s] = remote(
                    here, here, side_send.at[hop, k, s - 1], side_recv.at[hop, k, s - 1], 0, s
                )
    key_up, key_down, key_side = {}, {}, {}
    for hop in range(1, reach + 1):
        for copies, way in ((key_up, -1), (key_down, 1)):
            copies[hop] = remote(
                keys.at[reach + way * (hop - 1), sub], keys.at[reach + way * hop, sub],
                key_send.at[reach + way * hop, 0], key_recv.at[reach + way * hop, 0], -way, 0,
            )
    for hop in range(reach + 1):
        for s in range(1, subs):
            here = keys.at[reach + hop, sub]
            key_side[hop, s] = remote(
                here, here, key_send.at[reach + hop, s], key_recv.at[reach + hop, s], 0, s
            )

    key_up[1].start()
    key_down[1].start()
    for k in range(chunks):
        up[1, k].start()
        down[1, k].start()
    for k in range(chunks):
        for s in range(1, subs):
            side[0, k, s].start()
    for s in range(1, subs):
        key_side[0, s].start()

    unit_right[0, sub] = normalize(right[0, sub])
    for k in range(chunks):
        for s in range(1, subs):
            side[0, k, s].wait_recv()
    for s in range(1, subs):
        unit_right[0, lax.rem(sub + s, subs)] = normalize(right[0, lax.rem(sub + s, subs)])
        key_side[0, s].wait_recv()

    floor = jnp.float32(-1.0)
    wide = subs * rows
    best_row, best_col = {}, {}

    def compare(back, ahead):
        lhs = unit_right[0, sub] if back == 0 else unit_left[back - 1]
        rhs = unit_right[ahead].reshape(wide, width)
        scores = lax.dot_general(
            lhs, rhs, (((1,), (1,)), ((), ())), preferred_element_type=jnp.float32
        )
        row_key = jnp.broadcast_to(keys[reach - back, sub], (LANES, rows)).T
        col_key = jnp.concatenate([keys[reach + ahead, s] for s in range(subs)], axis=1)
        columns = []
        for start in range(0, wide, LANES):
            tile = scores[:, start : start + LANES]
            other = jnp.broadcast_to(col_key[:, start : start + LANES], (rows, LANES))
            same = jnp.where((row_key ^ other) < label_stride, tile, floor)
            earlier = other < row_key
            to_row = jnp.where(earlier, same, floor)
            best_row[back] = jnp.maximum(best_row[back], to_row) if back in best_row else to_row
            if ahead or back:
                columns.append(jnp.max(jnp.where(earlier, floor, same), axis=0, keepdims=True))
        if columns:
            column = jnp.concatenate(columns, axis=1)
            best_col[ahead] = (
                jnp.maximum(best_col[ahead], column) if ahead in best_col else column
            )

    def row_of(back):
        return jnp.max(best_row[back].T, axis=0, keepdims=True)

    pairs, last_row, last_col, late_rows, late_cols = plan(n, reach)
    row_slot = {back: 1 + i for i, back in enumerate(late_rows)}
    col_slot = {
        (ahead, s): 1 + len(late_rows) + i * subs + s
        for i, ahead in enumerate(late_cols) for s in range(subs)
    }
    row_copies, col_copies = [], []

    def run(i):
        back, ahead = pairs[i]
        compare(back, ahead)
        if back in late_rows and last_row[back] == i:
            table[place, sub, row_slot[back]] = row_of(back)
        elif back and last_row[back] == i:
            row_out[back - 1] = row_of(back)
            copy = remote(
                row_out.at[back - 1], row_in.at[back - 1],
                row_send.at[back - 1], row_recv.at[back - 1], -back, 0,
            )
            copy.start()
            row_copies.append(copy)
        if ahead in late_cols and last_col[ahead] == i:
            for s in range(subs):
                table[place, sub, col_slot[ahead, s]] = best_col[ahead][:, s * rows : (s + 1) * rows]
        elif ahead and last_col[ahead] == i:
            for s in range(subs):
                col_out[ahead - 1, s] = best_col[ahead][:, s * rows : (s + 1) * rows]
            for s in range(subs):
                target = lax.rem(sub + s, subs)
                copy = remote(
                    col_out.at[ahead - 1, target], col_in.at[ahead - 1, sub],
                    col_send.at[ahead - 1, s], col_recv.at[ahead - 1, s], ahead, s,
                )
                copy.start()
                col_copies.append(copy)

    run(0)
    done = 1
    rounds = n // 2
    for hop in range(1, reach + 1):
        for r in range(rounds * (hop - 1) // reach, rounds * hop // reach):
            for o, s in near:
                pl.semaphore_signal(
                    ready.at[r], inc=1, device_id=device(o, s), device_id_type=MESH
                )
            pl.semaphore_wait(ready.at[r], len(near))
        key_up[hop].wait_recv()
        key_down[hop].wait_recv()
        if hop < reach:
            key_up[hop + 1].start()
            key_down[hop + 1].start()
        for s in range(1, subs):
            key_side[hop, s].start()
        for k in range(chunks):
            up[hop, k].wait_recv()
            if hop < reach:
                up[hop + 1, k].start()
            down[hop, k].wait_recv()
            if hop < reach:
                down[hop + 1, k].start()
            for s in range(1, subs):
                side[hop, k, s].start()
            unit_left[hop - 1, span(k)] = normalize(left[hop - 1, span(k)])
            unit_right[hop, sub, span(k)] = normalize(right[hop, sub, span(k)])
            for s in range(1, subs):
                side[hop, k, s].wait_recv()
                there = lax.rem(sub + s, subs)
                unit_right[hop, there, span(k)] = normalize(right[hop, there, span(k)])
        for s in range(1, subs):
            key_side[hop, s].wait_recv()
        if hop == reach:
            for copy in row_copies + col_copies:
                copy.wait_recv()
            base = jnp.maximum(row_of(0), floor)
            for back in last_row:
                if back and back not in late_rows:
                    base = jnp.maximum(base, row_in[back - 1])
            for ahead in last_col:
                if ahead and ahead not in late_cols:
                    for s in range(subs):
                        base = jnp.maximum(base, col_in[ahead - 1, s])
            table[place, sub, 0] = base
        while done < len(pairs) and max(pairs[done]) <= hop:
            run(done)
            done += 1

    own = table.at[place, sub]
    table_copies = [
        remote(own, own, sum_send.at[o, s], sum_recv.at[o, s], o, s) for o, s in reversed(others)
    ]
    for copy in table_copies:
        copy.start()
    for copies in (up, down, side, key_up, key_down, key_side):
        for copy in copies.values():
            copy.wait_send()
    for copy in row_copies + col_copies:
        copy.wait_send()
    for copy in table_copies:
        copy.wait_recv()

    for q in range(n):
        for s in range(subs):
            value = table[q, s, 0]
            for back in late_rows:
                value = jnp.maximum(value, table[(q + back) % n, s, row_slot[back]])
            for ahead in late_cols:
                for t in range(subs):
                    value = jnp.maximum(value, table[(q - ahead) % n, t, col_slot[ahead, s]])
            maxima[q * subs + s] = value
    best_ref[...] = maxima[place * subs + sub].reshape(rows)
    best = maxima[...].reshape(n * subs, rows)
    scale = math.sqrt(width)
    index = jnp.full(best.shape, limit_ref[0], jnp.int32)
    limit = (2.0 + 0.5 * index.astype(jnp.float32)) / scale
    kept = jax.nn.sigmoid(2.0 * scale * (limit - best))
    total = jnp.sum(jnp.sum(kept, axis=0, keepdims=True), axis=1, keepdims=True)
    share_ref[...] = total / (n * subs * rows)
    for copy in table_copies:
        copy.wait_send()


def solution(mesh):
    n, subs = mesh.shape["blk"], mesh.shape["sub"]

    def on_device(embeddings, member_key, limit_index):
        rows, width = embeddings.shape
        reach = -(-(n // 2) // 2)
        chunks = 3 if rows % 48 == 0 else 1
        late_rows, late_cols = plan(n, reach)[3:]
        slots = 1 + len(late_rows) + len(late_cols) * subs
        dma = pltpu.SemaphoreType.DMA
        raw, f32, i32 = embeddings.dtype, jnp.float32, jnp.int32
        best, share = pl.pallas_call(
            functools.partial(kernel, n, subs, reach, chunks),
            out_shape=(
                jax.ShapeDtypeStruct((rows,), f32),
                jax.ShapeDtypeStruct((1, 1), f32),
            ),
            in_specs=[
                pl.BlockSpec(memory_space=pltpu.HBM),
                pl.BlockSpec(memory_space=pltpu.HBM),
                pl.BlockSpec(memory_space=pltpu.SMEM),
            ],
            out_specs=(
                pl.BlockSpec(memory_space=pltpu.VMEM),
                pl.BlockSpec(memory_space=pltpu.VMEM),
            ),
            scratch_shapes=[
                pltpu.VMEM((reach, rows, width), raw),
                pltpu.VMEM((reach + 1, subs, rows, width), raw),
                pltpu.VMEM((reach, rows, width), jnp.bfloat16),
                pltpu.VMEM((reach + 1, subs, rows, width), jnp.bfloat16),
                pltpu.VMEM((2 * reach + 1, subs, 1, rows), i32),
                pltpu.VMEM((reach, 1, rows), f32),
                pltpu.VMEM((reach, 1, rows), f32),
                pltpu.VMEM((reach, subs, 1, rows), f32),
                pltpu.VMEM((reach, subs, 1, rows), f32),
                pltpu.VMEM((n, subs, slots, 1, rows), f32),
                pltpu.VMEM((n * subs, 1, rows), f32),
                pltpu.SemaphoreType.REGULAR((n // 2,)),
                dma((2,)),
                dma((2 * reach + 1, subs)),
                dma((2 * reach + 1, subs)),
                dma((reach, chunks)),
                dma((reach, chunks)),
                dma((reach, chunks)),
                dma((reach, chunks)),
                dma((reach + 1, chunks, max(subs - 1, 1))),
                dma((reach + 1, chunks, max(subs - 1, 1))),
                dma((reach,)),
                dma((reach,)),
                dma((reach, subs)),
                dma((reach, subs)),
                dma((n, subs)),
                dma((n, subs)),
            ],
            compiler_params=pltpu.CompilerParams(
                collective_id=0,
                has_side_effects=True,
            ),
        )(embeddings, member_key.reshape(1, rows), limit_index)
        return best, share.reshape(1)

    in_specs = (P(("groups", "blk", "sub"), None), P(("groups", "blk", "sub")), P("groups"))
    out_specs = (P(("groups", "blk", "sub")), P("groups"))
    return jax.shard_map(
        on_device, mesh=mesh, in_specs=in_specs, out_specs=out_specs, check_vma=False
    )
```
